512 devices in a mesh: gx: 16 (over z), gy: 8 (over y, core), gz: 4 (over x).
Axes of the slice: x: 4, y: 4, z: 16, core: 2. Of those that a mesh axis runs over, the one named last changes fastest.
Arguments:
- displace: float32 [3, 64, 128, 512], P(None, 'gx', 'gy', 'gz'), may hold values from -4 to 4
- dir_a: float32 [3, 64, 128, 512], P(None, 'gx', 'gy', 'gz'), may hold values from -6 to 6
- dir_b: float32 [3, 64, 128, 512], P(None, 'gx', 'gy', 'gz'), may hold values from -6 to 6
- force: float32 [3, 64, 128, 512], P(None, 'gx', 'gy', 'gz'), may hold values from -6 to 6
- damage: float32 [64, 128, 512], P('gx', 'gy', 'gz'), may hold values from 0 to 0.9
- slip: float32 [12, 64, 128, 512], P(None, 'gx', 'gy', 'gz'), may hold values from -2 to 2
- resist: float32 [12, 64, 128, 512], P(None, 'gx', 'gy', 'gz'), may hold values from 0.5 to 2
- grains: int32 [64, 128, 512], P('gx', 'gy', 'gz'), may hold values from 0 to 63
- counts: int32 [64, 64, 4], P('gx', 'gy', 'gz'), may hold values from 8 to 40, as said below
- schmid_raw: float32 [64, 12, 9], replicated, may hold values from -3 to 3
Outputs:
- residual: float32 [3, 64, 128, 512], P(None, 'gx', 'gy', 'gz')
- tangent_a: float32 [3, 64, 128, 512], P(None, 'gx', 'gy', 'gz')
- tangent_b: float32 [3, 64, 128, 512], P(None, 'gx', 'gy', 'gz')
- slip_new: float32 [12, 64, 128, 512], P(None, 'gx', 'gy', 'gz')
- resist_new: float32 [12, 64, 128, 512], P(None, 'gx', 'gy', 'gz')
The draws below stay inside these ranges and needn't reach their ends.
Inputs may be any that keep to these rules, and one draw needn't show every extreme that they name: `counts`: each block is 2 x 128 points of one first-dimension index; heavy blocks form a band in the second dimension whose place changes with the third-dimension block.
All inputs are finite; a program needn't handle non-finite values.
Results may differ from the reference program's by a relative error of at most 0.0003.
Values sent between devices are 32-bit elements; how exact they have to be, the bound alone decides.
No kernel may reach another device: no remote copies, remote signals or barrier semaphores. Data moves between devices by JAX's collectives and lax.ppermute only.
A program may use at most 64 MiB of HBM per device.

```python
import math
import jax
import jax.numpy as jnp
from jax import lax

SLIP = 12
GRAINS = 64
SUBMAX = 40
BY = 2
BZ = 128
NX = 64
NY = 128
NZ = 512


def draw_counts(key, part):
    first, second, third, fourth = jax.random.split(key, 4)
    rows = NX
    columns = NY // BY
    layers = NZ // BZ
    centre = jax.random.randint(first, (), 0, columns)
    drift = jax.random.randint(second, (), columns // 8 + 1, columns // 2 + 2)
    column_index = jnp.arange(columns)[None, :, None]
    layer_index = jnp.arange(layers)[None, None, :]
    band = max(columns // 16, 1)
    centre_here = (centre + drift * layer_index) % columns
    offset = (column_index - centre_here) % columns
    distance = jnp.minimum(offset, columns - offset)
    near = jnp.broadcast_to(distance < band, (rows, columns, layers))
    heavy = jax.random.randint(third, (rows, columns, layers), 30, 41)
    light = jax.random.randint(fourth, (rows, columns, layers), 8, 14)
    result = jnp.where(near, heavy, light)
    result = result.at[0, centre, 0].set(40)
    result = result.at[rows - 1, (centre + columns // 2) % columns, layers - 1].set(8)
    return result.astype(jnp.int32)


def place_ends(entries, rng, least, largest):
    longest = entries.shape.index(max(entries.shape))
    spots = []
    for shift in (0, 1):
        where = [jax.random.randint(jax.random.fold_in(rng, axis), (), 0, length) for axis, length in enumerate(entries.shape)]
        where[longest] = (where[longest] + shift) % entries.shape[longest]
        spots.append(tuple(where))
    return entries.at[spots[0]].set(least).at[spots[1]].set(largest)


def level_of(stream_key, dims, shards, least, largest):
    loudness, own = 1.0, jax.random.fold_in(stream_key, 6)
    for position, blocks in shards:
        heights = jnp.exp(jax.random.uniform(jax.random.fold_in(own, position), (blocks,), jnp.float32, least / len(shards), largest / len(shards)))
        loudness = loudness * jnp.repeat(heights, dims[position] // blocks).reshape([-1 if axis == position else 1 for axis in range(len(dims))])
    return loudness


def bell_draw(stream_key, dims, scale, reach, cuts=(), held_as=jnp.bfloat16):
    factor_of = level_of(stream_key, dims, cuts, -0.22, 0.18) if cuts else 1.0
    array = jax.random.normal(stream_key, dims, jnp.float32) * scale * factor_of
    return jnp.minimum(jnp.maximum(array, -reach), reach).astype(held_as)


def setup_inputs(seed: int = 0) -> dict:
    streams_of = jax.random.split(jax.random.key(seed), 11)
    displace = bell_draw(streams_of[0], (3, NX, NY, NZ), 0.5, 4.0, ((1, 16), (2, 8), (3, 4)), jnp.float32)
    dir_a = bell_draw(streams_of[1], (3, NX, NY, NZ), 1.0, 6.0, ((1, 16), (2, 8), (3, 4)), jnp.float32)
    dir_b = bell_draw(streams_of[2], (3, NX, NY, NZ), 1.0, 6.0, ((1, 16), (2, 8), (3, 4)), jnp.float32)
    force = bell_draw(streams_of[3], (3, NX, NY, NZ), 1.0, 6.0, ((1, 16), (2, 8), (3, 4)), jnp.float32)
    damage = jnp.clip(0.9 * jax.random.uniform(streams_of[4], (NX, NY, NZ), jnp.float32) ** level_of(streams_of[4], (NX, NY, NZ), ((0, 16), (1, 8), (2, 4)), -0.2, 0.2), 0.0, 0.9)
    slip = bell_draw(streams_of[5], (SLIP, NX, NY, NZ), 0.3, 2.0, ((1, 16), (2, 8), (3, 4)), jnp.float32)
    resist = jnp.clip(jnp.exp(math.log(2.0) - 1.3862944 * jax.random.uniform(streams_of[6], (SLIP, NX, NY, NZ), jnp.float32) ** level_of(streams_of[6], (SLIP, NX, NY, NZ), ((1, 16), (2, 8), (3, 4)), -0.2, 0.2)), 0.5, 2.0)
    grains = place_ends(jax.random.randint(streams_of[7], (NX, NY, NZ), 0, GRAINS), jax.random.fold_in(streams_of[7], 1), 0, GRAINS - 1).astype(jnp.int32)
    counts = draw_counts(jax.random.fold_in(streams_of[10], 71), 0)
    schmid_raw = bell_draw(streams_of[9], (GRAINS, SLIP, 9), 0.4, 3.0, (), jnp.float32)
    return dict(displace=displace, dir_a=dir_a, dir_b=dir_b, force=force, damage=damage, slip=slip, resist=resist, grains=grains, counts=counts, schmid_raw=schmid_raw)


lame_first = 0.8
shear_twice = 1.0
rate_scale = 1.5
harden_rate = 0.3
total_time = 1.0
floor_stiff = 0.05
highest = lax.Precision.HIGHEST


def schmid_table(schmid_raw):
    matrix = schmid_raw.reshape(GRAINS, SLIP, 3, 3)
    symmetric = 0.5 * (matrix + jnp.swapaxes(matrix, 2, 3))
    trace_sum = symmetric[..., 0, 0] + symmetric[..., 1, 1] + symmetric[..., 2, 2]
    return symmetric - (trace_sum / 3.0)[..., None, None] * jnp.eye(3, dtype=jnp.float32)


def central(padded):
    along_x = (padded[:, 2:, 1:-1, 1:-1] - padded[:, :-2, 1:-1, 1:-1]) * 0.5
    along_y = (padded[:, 1:-1, 2:, 1:-1] - padded[:, 1:-1, :-2, 1:-1]) * 0.5
    along_z = (padded[:, 1:-1, 1:-1, 2:] - padded[:, 1:-1, 1:-1, :-2]) * 0.5
    return jnp.stack([along_x, along_y, along_z], axis=1)


def diverge(padded):
    gradients = central(padded)
    shaped = gradients.reshape((gradients.shape[0] // 9, 3, 3, 3) + gradients.shape[2:])
    result = shaped[:, :, 0, 0] + shaped[:, :, 1, 1] + shaped[:, :, 2, 2]
    return result.reshape((-1,) + gradients.shape[2:])


def elastic(strain, degrade):
    trace_sum = strain[0, 0] + strain[1, 1] + strain[2, 2]
    identity = jnp.eye(3, dtype=jnp.float32).reshape((3, 3) + (1,) * (strain.ndim - 2))
    return degrade * (lame_first * trace_sum * identity + shear_twice * strain)


def contract(schmid_here, tensor):
    return jnp.einsum('aij...,ij...->a...', schmid_here, tensor, precision=highest)


def combine(weights, schmid_here):
    return jnp.einsum('a...,aij...->ij...', weights, schmid_here, precision=highest)


def material(grad_u, grad_a, grad_b, damage, slip, resist, schmid_here, steps, turns):
    degrade = (1.0 - damage) ** 2 + floor_stiff
    strain = 0.5 * (grad_u + jnp.swapaxes(grad_u, 0, 1))
    time_step = total_time / steps.astype(jnp.float32)

    def stress_at(slip_now):
        return elastic(strain - combine(slip_now, schmid_here), degrade)

    def substep(turn_index, state_pair):
        slip_now, resist_now = state_pair
        resolved = contract(schmid_here, stress_at(slip_now))
        slip_rate = rate_scale * jnp.tanh(resolved / resist_now)
        active = turn_index < steps
        slip_next = jnp.where(active, slip_now + time_step * slip_rate, slip_now)
        resist_next = jnp.where(active, resist_now + time_step * harden_rate * jnp.sum(jnp.abs(slip_rate), axis=0), resist_now)
        return slip_next, resist_next

    slip, resist = lax.fori_loop(0, turns, substep, (slip, resist))
    stress = stress_at(slip)
    ratio = jnp.tanh(contract(schmid_here, stress) / resist)
    softening = total_time * rate_scale * (1.0 - ratio * ratio) / resist

    def fluxes(grad_v):
        elastic_part = elastic(0.5 * (grad_v + jnp.swapaxes(grad_v, 0, 1)), degrade)
        projected = contract(schmid_here, elastic_part)
        return elastic_part - degrade * shear_twice * combine(softening * projected, schmid_here)

    return stress, fluxes(grad_a), fluxes(grad_b), slip, resist


def reference(displace, dir_a, dir_b, force, damage, slip, resist, grains, counts, schmid_raw):
    fields = jnp.concatenate([displace, dir_a, dir_b], 0)
    gradients = central(jnp.pad(fields, ((0, 0), (1, 1), (1, 1), (1, 1))))
    gradients = gradients.reshape(3, 3, 3, NX, NY, NZ)
    table = schmid_table(schmid_raw)
    steps = jnp.repeat(jnp.repeat(counts, BY, axis=1), BZ, axis=2)

    def one_slab(column):
        grad_here = lax.dynamic_index_in_dim(gradients, column, 3, keepdims=False)
        schmid_here = jnp.transpose(table[grains[column]], (2, 3, 4, 0, 1))
        return material(grad_here[0], grad_here[1], grad_here[2], damage[column], slip[:, column], resist[:, column], schmid_here, steps[column], SUBMAX)

    stress, flux_a, flux_b, slip_out, resist_out = lax.map(one_slab, jnp.arange(NX, dtype=jnp.int32))
    stress = jnp.moveaxis(stress, 0, 2).reshape(9, NX, NY, NZ)
    flux_a = jnp.moveaxis(flux_a, 0, 2).reshape(9, NX, NY, NZ)
    flux_b = jnp.moveaxis(flux_b, 0, 2).reshape(9, NX, NY, NZ)
    widths = ((0, 0), (1, 1), (1, 1), (1, 1))
    residual = diverge(jnp.pad(stress, widths)) + force
    tangent_a = diverge(jnp.pad(flux_a, widths))
    tangent_b = diverge(jnp.pad(flux_b, widths))
    return residual, tangent_a, tangent_b, jnp.moveaxis(slip_out, 0, 1), jnp.moveaxis(resist_out, 0, 1)
```

```python
import functools
import math

import jax
import jax.numpy as jnp
from jax import lax
from jax.experimental import pallas as pl
from jax.experimental.pallas import tpu as pltpu
from jax.sharding import PartitionSpec as P

SLIP = 12
GRAINS = 64
DEV = 5
WIDE = 2
LANES = 128
VMEM_LIMIT = 12 * 1024 * 1024


lame_first = 0.8
rate_scale = 1.5
harden_rate = 0.3
floor_stiff = 0.05

RT2 = math.sqrt(2.0)
RT6 = math.sqrt(6.0)


def entries(system):
    return range(min(system + 1, DEV))


SLOTS = [(a, c) for a in range(SLIP) for c in entries(a)]
SLOT_OF = {pair: k for k, pair in enumerate(SLOTS)}


def total(terms):
    terms = list(terms)
    while len(terms) > 1:
        terms = [terms[i] + terms[i + 1] if i + 1 < len(terms) else terms[i] for i in range(0, len(terms), 2)]
    return terms[0]


def chain(terms):
    terms = list(terms)
    acc = terms[0]
    for term in terms[1:]:
        acc = acc + term
    return acc


def pack_lane(tiles, lane):
    at = lax.broadcasted_iota(jnp.int32, (8, LANES), 1)
    packed = jnp.zeros((8, LANES), jnp.float32)
    for k, tile in enumerate(tiles):
        shift = (k - lane) % LANES
        moved = pltpu.roll(tile, shift, 1) if shift else tile
        packed = jnp.where(at == k, moved, packed)
    return packed


def parity():
    return lax.rem(lax.axis_index("gy"), 2)


def faces_kernel(u_hbm, a_hbm, b_hbm, fields, xlo, xhi, yeven, yodd, zlo, zhi, sem):
    nx, ny = fields.shape[1], fields.shape[2]
    odd = parity()
    row_even, row_odd = (1 - odd) * (ny - 1), odd * (ny - 1)
    copies = [
        pltpu.make_async_copy(ref, fields.at[pl.ds(3 * f, 3)], sem.at[f]) for f, ref in enumerate((u_hbm, a_hbm, b_hbm))
    ]
    for copy in copies:
        copy.start()
    tiles = []
    for n in range(9):
        if n % 3 == 0:
            copies[n // 3].wait()
        xlo[n] = fields[n, 0]
        xhi[n] = fields[n, nx - 1]
        for x in range(nx):
            row = n * nx + x
            yeven[pl.ds(row, 1), :] = fields[n, x, pl.ds(row_even, 1), :]
            yodd[pl.ds(row, 1), :] = fields[n, x, pl.ds(row_odd, 1), :]
            for h in range(ny // 8):
                tiles.append(fields[n, x, pl.ds(8 * h, 8), :])
    zlo[...] = pack_lane(tiles, 0)
    zhi[...] = pack_lane(tiles, LANES - 1)


def tile_counts(count_ref, x, h):
    row_at = lax.broadcasted_iota(jnp.int32, (8, LANES), 0)
    numbers = [count_ref[x, 0, 4 * h + j] for j in range(4)]
    upper = jnp.where(row_at < 2, numbers[0], numbers[1])
    lower = jnp.where(row_at < 6, numbers[2], numbers[3])
    return jnp.where(row_at < 4, upper, lower)


def stiffness(damage):
    undamaged = 1.0 - damage
    return undamaged * undamaged + floor_stiff


def table_kernel(raw_hbm, *refs):
    sources, (rows_ref, turn_ref), targets = refs[:4], refs[4:6], refs[6:10]
    raw_ref, wide_ref, sem = refs[10:]
    grain_ref = targets[3]
    nx, ny = grain_ref.shape[0], grain_ref.shape[1]
    first = pltpu.make_async_copy(raw_hbm, raw_ref, sem.at[4])
    first.start()
    copies = [pltpu.make_async_copy(source, target, sem.at[k]) for k, (source, target) in enumerate(zip(sources, targets))]
    for copy in copies:
        copy.start()
    wide_ref[...] = jnp.zeros_like(wide_ref)
    first.wait()
    wide_ref[:, pl.ds(0, SLIP), pl.ds(0, GRAINS)] = raw_ref[...]
    comp = [wide_ref[i] for i in range(9)]
    base = [
        (comp[0] - comp[4]) * (1.0 / RT2),
        (2.0 * comp[8] - comp[0] - comp[4]) * (1.0 / RT6),
        (comp[1] + comp[3]) * (1.0 / RT2),
        (comp[2] + comp[6]) * (1.0 / RT2),
        (comp[5] + comp[7]) * (1.0 / RT2),
    ]
    row_at = lax.broadcasted_iota(jnp.int32, (24, LANES), 0)
    both = []
    for c in range(DEV):
        both.append(jnp.where(row_at == 16 + c, 1.0, base[c]))
    for k in range(DEV - 1):
        for j in range(k + 1, DEV):
            first, second = both[k][k : k + 1], both[j][k : k + 1]
            square = first * first + second * second
            good = square > 0.0
            scale = lax.rsqrt(jnp.where(good, square, 1.0))
            cosine = jnp.where(good, first * scale, 1.0)
            sine = jnp.where(good, second * scale, 0.0)
            both[k], both[j] = cosine * both[k] + sine * both[j], cosine * both[j] - sine * both[k]
    for copy in copies:
        copy.wait()
    for x in range(nx):
        for h in range(ny // 8):
            rows = pl.ds(8 * h, 8)
            ids = grain_ref[x, rows, :]

            def look(row):
                spread = jnp.broadcast_to(row, (8, LANES))
                return jnp.take_along_axis(spread, ids, axis=1, mode="promise_in_bounds")

            for k, (a, c) in enumerate(SLOTS):
                rows_ref[k, x, rows, :] = look(both[c][a : a + 1])
            for c in range(DEV):
                for d in range(DEV):
                    turn_ref[DEV * c + d, x, rows, :] = look(both[c][16 + d : 17 + d])


def sort_halos(odd, yeven, yodd, ylo, yhi):
    upper = odd == 0
    yhi[...] = jnp.where(upper, yeven[...], yodd[...])
    ylo[...] = jnp.where(upper, yodd[...], yeven[...])


def gradient_parts(field, halos, f, x, h):
    xlo, xhi, ylo, yhi, zlo, zhi = halos
    nx, ny = field.shape[1], field.shape[2]
    row_at = lax.broadcasted_iota(jnp.int32, (8, LANES), 0)
    lane_at = lax.broadcasted_iota(jnp.int32, (8, LANES), 1)
    out = []
    for c in range(3):
        n = 3 * f + c
        here = field[n, x, pl.ds(8 * h, 8), :]
        ahead = field[n, x + 1, pl.ds(8 * h, 8), :] if x + 1 < nx else xhi[n, pl.ds(8 * h, 8), :]
        behind = field[n, x - 1, pl.ds(8 * h, 8), :] if x > 0 else xlo[n, pl.ds(8 * h, 8), :]
        row = n * nx + x
        if 8 * h + 8 < ny:
            over = field[n, x, pl.ds(8 * h + 1, 8), :]
        else:
            edge = jnp.broadcast_to(yhi[pl.ds(row, 1), :], (8, LANES))
            over = jnp.where(row_at == 7, edge, pltpu.roll(here, 7, 0))
        if h > 0:
            under = field[n, x, pl.ds(8 * h - 1, 8), :]
        else:
            edge = jnp.broadcast_to(ylo[pl.ds(row, 1), :], (8, LANES))
            under = jnp.where(row_at == 0, edge, pltpu.roll(here, 1, 0))
        k = row * (ny // 8) + h
        top = pltpu.roll(zhi[...], (LANES - 1 - k) % LANES, 1)
        low = pltpu.roll(zlo[...], (LANES - k) % LANES, 1) if k else zlo[...]
        right = jnp.where(lane_at == LANES - 1, top, pltpu.roll(here, LANES - 1, 1))
        left = jnp.where(lane_at == 0, low, pltpu.roll(here, 1, 1))
        out.append((ahead - behind, over - under, right - left))
    return out


def strain_parts(field, halos, f, x0, h):
    per = []
    for x in range(x0, x0 + WIDE):
        g = gradient_parts(field, halos, f, x, h)
        trace = (g[0][0] + g[1][1] + g[2][2]) * 0.5
        per.append(
            (
                trace,
                (g[0][0] - g[1][1]) * (0.5 / RT2),
                (2.0 * g[2][2] - g[0][0] - g[1][1]) * (0.5 / RT6),
                (g[0][1] + g[1][0]) * (0.5 / RT2),
                (g[0][2] + g[2][0]) * (0.5 / RT2),
                (g[1][2] + g[2][1]) * (0.5 / RT2),
            )
        )
    stacked = [jnp.stack([p[i] for p in per], 0) for i in range(6)]
    return stacked[0], stacked[1:]


def full_tensor(mean, dev):
    side = dev[1] * (1.0 / RT6)
    return [
        mean - side + dev[0] * (1.0 / RT2),
        mean - side - dev[0] * (1.0 / RT2),
        mean + dev[1] * (2.0 / RT6),
        dev[2] * (1.0 / RT2),
        dev[3] * (1.0 / RT2),
        dev[4] * (1.0 / RT2),
    ]


SYM = ((0, 3, 4), (3, 1, 5), (4, 5, 2))


def material_kernel(
    count_ref, fields, xlo, xhi, yeven, yodd, zlo, zhi, damage_ref, slip_ref, resist_ref, rows_ref, turn_ref,
    slip_hbm, resist_hbm, tensor_out, oxlo, oxhi, oyeven, oyodd, ozlo, ozhi,
    ylo, yhi, scaled_ref, sums_ref, slip_out, resist_out, sent,
):
    nx, ny = fields.shape[1], fields.shape[2]
    odd = parity()
    row_even, row_odd = (1 - odd) * (ny - 1), odd * (ny - 1)
    sort_halos(odd, yeven, yodd, ylo, yhi)
    halos = (xlo, xhi, ylo, yhi, zlo, zhi)
    copies = []
    for x0 in range(0, nx, WIDE):
        for h in range(ny // 8):
            spot = (pl.ds(x0, WIDE), pl.ds(8 * h, 8), slice(None))
            least = most = count_ref[x0, 0, 4 * h]
            for x in range(x0, x0 + WIDE):
                for j in range(4):
                    least = jnp.minimum(least, count_ref[x, 0, 4 * h + j])
                    most = jnp.maximum(most, count_ref[x, 0, 4 * h + j])
            steps = [tile_counts(count_ref, x, h) for x in range(x0, x0 + WIDE)]
            steps = jnp.stack(steps, 0)
            count = steps.astype(jnp.float32)
            time_step = 1.0 / count
            degrade = stiffness(damage_ref[spot])
            scale = jnp.sqrt(rate_scale * degrade * time_step)
            for k in range(len(SLOTS)):
                scaled_ref[k] = rows_ref[(k,) + spot] * scale

            def entry(a, c):
                return scaled_ref[SLOT_OF[(a, c)]]

            def turned(vector):
                return [total(turn_ref[(DEV * c + d,) + spot] * vector[d] for d in range(DEV)) for c in range(DEV)]

            def returned(vector):
                return [total(turn_ref[(DEV * c + d,) + spot] * vector[c] for c in range(DEV)) for d in range(DEV)]

            def project(vector, a):
                return total(entry(a, c) * vector[c] for c in entries(a))

            def gather(weights, c):
                return chain(entry(a, c) * weights[a] for a in range(SLIP) if c in entries(a))

            trace_u, strain = strain_parts(fields, halos, 0, x0, h)
            strain = turned(strain)
            lift = jnp.sqrt(degrade * count * (1.0 / rate_scale))
            start_slip = [slip_ref[(a,) + spot] for a in range(SLIP)]
            share = count * (1.0 / rate_scale)
            drive = tuple(lift * strain[c] - share * gather(start_slip, c) for c in range(DEV))
            grow = (rate_scale * harden_rate) * time_step
            zero = jnp.zeros_like(count)

            def rates(driving, growth):
                return [jnp.tanh(project(driving, a) / (resist_ref[(a,) + spot] + growth)) for a in range(SLIP)]

            def substep(_, state):
                driving, growth = state
                rate = rates(driving, growth)
                for a in range(SLIP):
                    sums_ref[a] = sums_ref[a] + rate[a]
                growth = growth + grow * total(jnp.abs(r) for r in rate)
                driving = tuple(driving[c] - gather(rate, c) for c in range(DEV))
                return driving, growth

            def masked(turn, state):
                driving, growth = state
                live = turn < steps
                return substep(turn, (tuple(jnp.where(live, d, 0.0) for d in driving), growth))

            for a in range(SLIP):
                sums_ref[a] = zero
            state = lax.fori_loop(0, least, substep, (drive, zero))
            _, growth = lax.fori_loop(least, most, masked, state)
            sums = [sums_ref[a] for a in range(SLIP)]
            for a in range(SLIP):
                slip_out[(a,) + spot] = slip_ref[(a,) + spot] + (rate_scale * time_step) * sums[a]
                resist_out[(a,) + spot] = resist_ref[(a,) + spot] + growth
            group = x0 // WIDE * (ny // 8) + h
            for kind, (held, away) in enumerate(((slip_out, slip_hbm), (resist_out, resist_hbm))):
                part = (slice(None),) + spot
                copy = pltpu.make_async_copy(held.at[part], away.at[part], sent.at[kind, group])
                copy.start()
                copies.append(copy)
            drive = [drive[c] - gather(sums, c) for c in range(DEV)]
            stress = returned([scale * d for d in drive])
            soft = []
            for a, ratio in enumerate(rates(drive, growth)):
                soft.append((1.0 - ratio * ratio) / (resist_ref[(a,) + spot] + growth))
            bulk = degrade * (lame_first + 1.0 / 3.0)
            tensors = [full_tensor(bulk * trace_u, stress)]
            for f in (1, 2):
                trace_v, dev = strain_parts(fields, halos, f, x0, h)
                dev = [degrade * d for d in dev]
                local = turned(dev)
                weights = [soft[a] * project(local, a) for a in range(SLIP)]
                loss = returned([count * gather(weights, c) for c in range(DEV)])
                tensors.append(full_tensor(bulk * trace_v, [d - q for d, q in zip(dev, loss)]))
            for f in range(3):
                for s in range(6):
                    tensor_out[(6 * f + s,) + spot] = tensors[f][s]
    tiles = []
    for f in range(3):
        for i in range(3):
            n = 3 * f + i
            sx, sy, sz = (6 * f + SYM[i][j] for j in range(3))
            oxlo[n] = tensor_out[sx, 0]
            oxhi[n] = tensor_out[sx, nx - 1]
            for x in range(nx):
                oyeven[pl.ds(n * nx + x, 1), :] = tensor_out[sy, x, pl.ds(row_even, 1), :]
                oyodd[pl.ds(n * nx + x, 1), :] = tensor_out[sy, x, pl.ds(row_odd, 1), :]
                for h in range(ny // 8):
                    tiles.append(tensor_out[sz, x, pl.ds(8 * h, 8), :])
    ozlo[...] = pack_lane(tiles, 0)
    ozhi[...] = pack_lane(tiles, LANES - 1)
    for copy in copies:
        copy.wait()


def diverge_kernel(
    tensor_ref, xlo, xhi, yeven, yodd, zlo, zhi, force_ref, residual, tangent_a, tangent_b, ylo, yhi
):
    nx, ny = tensor_ref.shape[1], tensor_ref.shape[2]
    sort_halos(parity(), yeven, yodd, ylo, yhi)
    row_at = lax.broadcasted_iota(jnp.int32, (8, LANES), 0)
    lane_at = lax.broadcasted_iota(jnp.int32, (8, LANES), 1)
    for f, out in enumerate((residual, tangent_a, tangent_b)):
        for i in range(3):
            n = 3 * f + i
            sx, sy, sz = (6 * f + SYM[i][j] for j in range(3))
            for x in range(nx):
                for h in range(ny // 8):
                    rows = pl.ds(8 * h, 8)
                    ahead = tensor_ref[sx, x + 1, rows, :] if x + 1 < nx else xhi[n, rows, :]
                    behind = tensor_ref[sx, x - 1, rows, :] if x > 0 else xlo[n, rows, :]
                    row = n * nx + x
                    here = tensor_ref[sy, x, rows, :]
                    if 8 * h + 8 < ny:
                        over = tensor_ref[sy, x, pl.ds(8 * h + 1, 8), :]
                    else:
                        edge = jnp.broadcast_to(yhi[pl.ds(row, 1), :], (8, LANES))
                        over = jnp.where(row_at == 7, edge, pltpu.roll(here, 7, 0))
                    if h > 0:
                        under = tensor_ref[sy, x, pl.ds(8 * h - 1, 8), :]
                    else:
                        edge = jnp.broadcast_to(ylo[pl.ds(row, 1), :], (8, LANES))
                        under = jnp.where(row_at == 0, edge, pltpu.roll(here, 1, 0))
                    k = row * (ny // 8) + h
                    here = tensor_ref[sz, x, rows, :]
                    top = pltpu.roll(zhi[...], (LANES - 1 - k) % LANES, 1)
                    low = pltpu.roll(zlo[...], (LANES - k) % LANES, 1) if k else zlo[...]
                    right = jnp.where(lane_at == LANES - 1, top, pltpu.roll(here, LANES - 1, 1))
                    left = jnp.where(lane_at == 0, low, pltpu.roll(here, 1, 1))
                    value = 0.5 * ((ahead - behind) + (over - under) + (right - left))
                    if f == 0:
                        value = value + force_ref[i, x, rows, :]
                    out[i, x, rows, :] = value


def exchange(faces):
    xlo, xhi, yeven, yodd, zlo, zhi = faces

    def shift(value, axis, step):
        size = lax.axis_size(axis)
        return lax.ppermute(value, axis, [(i, i + step) for i in range(size) if 0 <= i + step < size])

    def swap(value, axis, first):
        size = lax.axis_size(axis)
        pairs = [(i, i + 1) for i in range(first, size - 1, 2)]
        return lax.ppermute(value, axis, pairs + [(j, i) for i, j in pairs])

    yeven = swap(yeven, "gy", 0)
    xlo, xhi = shift(xhi, "gx", 1), shift(xlo, "gx", -1)
    zlo, zhi = shift(zhi, "gz", 1), shift(zlo, "gz", -1)
    yodd = swap(yodd, "gy", 1)
    return xlo, xhi, yeven, yodd, zlo, zhi


def in_hbm(value):
    return pltpu.with_memory_space_constraint(value, pltpu.HBM)


def shaped(*dims):
    return jax.ShapeDtypeStruct(dims, jnp.float32)


def on_device(displace, dir_a, dir_b, force, damage, slip, resist, grains, counts, schmid_raw):
    nx, ny, nz = damage.shape
    face_shapes = [shaped(9, ny, nz)] * 2 + [shaped(9 * nx, nz)] * 2 + [shaped(8, nz)] * 2
    vmem = pl.BlockSpec(memory_space=pltpu.VMEM)
    smem = pl.BlockSpec(memory_space=pltpu.SMEM)
    hbm = pl.BlockSpec(memory_space=pltpu.HBM)
    params = pltpu.CompilerParams(vmem_limit_bytes=VMEM_LIMIT)
    fields, *faces = pl.pallas_call(
        faces_kernel,
        out_shape=[shaped(9, nx, ny, nz)] + face_shapes,
        in_specs=[hbm] * 3,
        out_specs=[vmem] * 7,
        scratch_shapes=[pltpu.SemaphoreType.DMA((3,))],
        compiler_params=params,
        name="faces",
    )(*(in_hbm(v) for v in (displace, dir_a, dir_b)))
    points = [in_hbm(v) for v in (damage, slip, resist, grains)]
    number = in_hbm(jnp.transpose(counts, (0, 2, 1)))
    rows, turn, *points = pl.pallas_call(
        table_kernel,
        out_shape=[shaped(len(SLOTS), nx, ny, nz), shaped(DEV * DEV, nx, ny, nz)]
        + [jax.ShapeDtypeStruct(p.shape, p.dtype) for p in points],
        in_specs=[hbm] * 5,
        out_specs=[vmem] * 6,
        scratch_shapes=[
            pltpu.VMEM((9, SLIP, GRAINS), jnp.float32),
            pltpu.VMEM((9, 24, LANES), jnp.float32),
            pltpu.SemaphoreType.DMA((5,)),
        ],
        compiler_params=params,
        name="table",
    )(in_hbm(jnp.transpose(schmid_raw, (2, 1, 0))), *points)
    halos = exchange(faces)
    groups = nx // WIDE * (ny // 8)
    outs = pl.pallas_call(
        material_kernel,
        out_shape=[shaped(SLIP, nx, ny, nz)] * 2 + [shaped(18, nx, ny, nz)] + face_shapes,
        in_specs=[smem] + [vmem] * 12,
        out_specs=[hbm] * 2 + [vmem] * 7,
        scratch_shapes=[
            pltpu.VMEM((9 * nx, nz), jnp.float32),
            pltpu.VMEM((9 * nx, nz), jnp.float32),
            pltpu.VMEM((len(SLOTS), WIDE, 8, LANES), jnp.float32),
            pltpu.VMEM((SLIP, WIDE, 8, LANES), jnp.float32),
            pltpu.VMEM((SLIP, nx, ny, nz), jnp.float32),
            pltpu.VMEM((SLIP, nx, ny, nz), jnp.float32),
            pltpu.SemaphoreType.DMA((2, groups)),
        ],
        compiler_params=params,
        name="material",
    )(number, fields, *halos, *points[:3], rows, turn)
    slip_new, resist_new, tensors = outs[:3]
    halos = exchange(outs[3:])
    residual, tangent_a, tangent_b = pl.pallas_call(
        diverge_kernel,
        out_shape=[shaped(3, nx, ny, nz)] * 3,
        in_specs=[vmem] * 8,
        out_specs=[vmem] * 3,
        scratch_shapes=[pltpu.VMEM((9 * nx, nz), jnp.float32)] * 2,
        compiler_params=params,
        name="diverge",
    )(tensors, *halos, force)
    return residual, tangent_a, tangent_b, slip_new, resist_new


def solution(mesh):
    field = P(None, "gx", "gy", "gz")
    point = P("gx", "gy", "gz")
    return jax.shard_map(
        on_device,
        mesh=mesh,
        in_specs=(field, field, field, field, point, field, field, point, point, P()),
        out_specs=(field,) * 5,
        check_vma=False,
    )
```

```python
import math

import jax
import jax.numpy as jnp
from jax import lax
from jax.experimental import pallas as pl
from jax.experimental.pallas import tpu as pltpu
from jax.sharding import PartitionSpec as P

SLIP = 12
GRAINS = 64
DEV = 5
WIDE = 2
UNROLL = 4
NAMES = ("xlo", "xhi", "yeven", "yodd", "zlo", "zhi")
ORDER_FIRST = ("xlo", "xhi", "yeven", "yodd", "zlo", "zhi")
ORDER_LAST = ("yeven", "xlo", "xhi", "zlo", "zhi", "yodd")
UNROLL_MASKED = 2
LANES = 128
VMEM_LIMIT = 12 * 1024 * 1024


lame_first = 0.8
rate_scale = 1.5
harden_rate = 0.3
floor_stiff = 0.05

RT2 = math.sqrt(2.0)
RT6 = math.sqrt(6.0)


def entries(system):
    return range(min(system + 1, DEV))


SLOTS = [(a, c) for a in range(SLIP) for c in entries(a)]
SLOT_OF = {pair: k for k, pair in enumerate(SLOTS)}


def total(terms):
    terms = list(terms)
    while len(terms) > 1:
        terms = [terms[i] + terms[i + 1] if i + 1 < len(terms) else terms[i] for i in range(0, len(terms), 2)]
    return terms[0]


def chain(terms):
    terms = list(terms)
    acc = terms[0]
    for term in terms[1:]:
        acc = acc + term
    return acc


def pack_lane(tiles, lane):
    at = lax.broadcasted_iota(jnp.int32, (8, LANES), 1)
    packed = jnp.zeros((8, LANES), jnp.float32)
    for k, tile in enumerate(tiles):
        shift = (k - lane) % LANES
        moved = pltpu.roll(tile, shift, 1) if shift else tile
        packed = jnp.where(at == k, moved, packed)
    return packed


def parity():
    return lax.rem(lax.axis_index("gy"), 2)


def in_order(refs, order):
    return [refs[order.index(name)] for name in NAMES]


def faces_kernel(u_hbm, a_hbm, b_hbm, fields, *refs):
    xlo, xhi, yeven, yodd, zlo, zhi = in_order(refs[:6], ORDER_FIRST)
    sem = refs[6]
    nx, ny = fields.shape[1], fields.shape[2]
    odd = parity()
    row_even, row_odd = (1 - odd) * (ny - 1), odd * (ny - 1)
    copies = [
        pltpu.make_async_copy(ref, fields.at[pl.ds(3 * f, 3)], sem.at[f]) for f, ref in enumerate((u_hbm, a_hbm, b_hbm))
    ]
    for copy in copies:
        copy.start()
    tiles = []
    for n in range(9):
        if n % 3 == 0:
            copies[n // 3].wait()
        xlo[n] = fields[n, 0]
        xhi[n] = fields[n, nx - 1]
        for x in range(nx):
            row = n * nx + x
            yeven[pl.ds(row, 1), :] = fields[n, x, pl.ds(row_even, 1), :]
            yodd[pl.ds(row, 1), :] = fields[n, x, pl.ds(row_odd, 1), :]
            for h in range(ny // 8):
                tiles.append(fields[n, x, pl.ds(8 * h, 8), :])
    zlo[...] = pack_lane(tiles, 0)
    zhi[...] = pack_lane(tiles, LANES - 1)


def tile_counts(count_ref, x, h):
    row_at = lax.broadcasted_iota(jnp.int32, (8, LANES), 0)
    numbers = [count_ref[x, 0, 4 * h + j] for j in range(4)]
    upper = jnp.where(row_at < 2, numbers[0], numbers[1])
    lower = jnp.where(row_at < 6, numbers[2], numbers[3])
    return jnp.where(row_at < 4, upper, lower)


def stiffness(damage):
    undamaged = 1.0 - damage
    return undamaged * undamaged + floor_stiff


def table_kernel(raw_hbm, *refs):
    sources, count_hbm, (rows_ref, turn_ref, past_ref, steps_ref) = refs[:4], refs[4], refs[5:9]
    targets, count_out, raw_ref, wide_ref, count_ref, sem = refs[9:13], refs[13], refs[14], refs[15], refs[16], refs[17]
    _, slip_ref, _, grain_ref = targets
    numbers = [
        pltpu.make_async_copy(count_hbm, count_ref, sem.at[5]),
        pltpu.make_async_copy(count_hbm, count_out, sem.at[6]),
    ]
    for copy in numbers:
        copy.start()
    nx, ny = grain_ref.shape[0], grain_ref.shape[1]
    first = pltpu.make_async_copy(raw_hbm, raw_ref, sem.at[4])
    first.start()
    copies = [pltpu.make_async_copy(source, target, sem.at[k]) for k, (source, target) in enumerate(zip(sources, targets))]
    for copy in copies:
        copy.start()
    wide_ref[...] = jnp.zeros_like(wide_ref)
    first.wait()
    wide_ref[:, pl.ds(0, SLIP), pl.ds(0, GRAINS)] = raw_ref[...]
    comp = [wide_ref[i] for i in range(9)]
    base = [
        (comp[0] - comp[4]) * (1.0 / RT2),
        (2.0 * comp[8] - comp[0] - comp[4]) * (1.0 / RT6),
        (comp[1] + comp[3]) * (1.0 / RT2),
        (comp[2] + comp[6]) * (1.0 / RT2),
        (comp[5] + comp[7]) * (1.0 / RT2),
    ]
    row_at = lax.broadcasted_iota(jnp.int32, (24, LANES), 0)
    both = []
    for c in range(DEV):
        both.append(jnp.where(row_at == 16 + c, 1.0, base[c]))
    for k in range(DEV - 1):
        for j in range(k + 1, DEV):
            first, second = both[k][k : k + 1], both[j][k : k + 1]
            square = first * first + second * second
            good = square > 0.0
            scale = lax.rsqrt(jnp.where(good, square, 1.0))
            cosine = jnp.where(good, first * scale, 1.0)
            sine = jnp.where(good, second * scale, 0.0)
            both[k], both[j] = cosine * both[k] + sine * both[j], cosine * both[j] - sine * both[k]
    for copy in copies + numbers:
        copy.wait()
    for x in range(nx):
        for h in range(ny // 8):
            rows = pl.ds(8 * h, 8)
            ids = grain_ref[x, rows, :]

            def look(row):
                spread = jnp.broadcast_to(row, (8, LANES))
                return jnp.take_along_axis(spread, ids, axis=1, mode="promise_in_bounds")

            steps_ref[x, rows, :] = tile_counts(count_ref, x, h)
            past = [None] * DEV
            for k, (a, c) in enumerate(SLOTS):
                value = look(both[c][a : a + 1])
                rows_ref[k, x, rows, :] = value
                term = slip_ref[a, x, rows, :] * value
                past[c] = term if past[c] is None else past[c] + term
            for c in range(DEV):
                past_ref[c, x, rows, :] = past[c]
            for c in range(DEV):
                for d in range(DEV):
                    turn_ref[DEV * c + d, x, rows, :] = look(both[c][16 + d : 17 + d])


def sort_halos(odd, yeven, yodd, ylo, yhi):
    upper = odd == 0
    yhi[...] = jnp.where(upper, yeven[...], yodd[...])
    ylo[...] = jnp.where(upper, yodd[...], yeven[...])


def gradient_parts(field, halos, f, x, h):
    xlo, xhi, ylo, yhi, zlo, zhi = halos
    nx, ny = field.shape[1], field.shape[2]
    row_at = lax.broadcasted_iota(jnp.int32, (8, LANES), 0)
    lane_at = lax.broadcasted_iota(jnp.int32, (8, LANES), 1)
    out = []
    for c in range(3):
        n = 3 * f + c
        here = field[n, x, pl.ds(8 * h, 8), :]
        ahead = field[n, x + 1, pl.ds(8 * h, 8), :] if x + 1 < nx else xhi[n, pl.ds(8 * h, 8), :]
        behind = field[n, x - 1, pl.ds(8 * h, 8), :] if x > 0 else xlo[n, pl.ds(8 * h, 8), :]
        row = n * nx + x
        if 8 * h + 8 < ny:
            over = field[n, x, pl.ds(8 * h + 1, 8), :]
        else:
            edge = jnp.broadcast_to(yhi[pl.ds(row, 1), :], (8, LANES))
            over = jnp.where(row_at == 7, edge, pltpu.roll(here, 7, 0))
        if h > 0:
            under = field[n, x, pl.ds(8 * h - 1, 8), :]
        else:
            edge = jnp.broadcast_to(ylo[pl.ds(row, 1), :], (8, LANES))
            under = jnp.where(row_at == 0, edge, pltpu.roll(here, 1, 0))
        k = row * (ny // 8) + h
        top = pltpu.roll(zhi[...], (LANES - 1 - k) % LANES, 1)
        low = pltpu.roll(zlo[...], (LANES - k) % LANES, 1)
        right = jnp.where(lane_at == LANES - 1, top, pltpu.roll(here, LANES - 1, 1))
        left = jnp.where(lane_at == 0, low, pltpu.roll(here, 1, 1))
        out.append((ahead - behind, over - under, right - left))
    return out


def strain_parts(field, halos, f, x0, h):
    per = []
    for x in range(x0, x0 + WIDE):
        g = gradient_parts(field, halos, f, x, h)
        trace = (g[0][0] + g[1][1] + g[2][2]) * 0.5
        per.append(
            (
                trace,
                (g[0][0] - g[1][1]) * (0.5 / RT2),
                (2.0 * g[2][2] - g[0][0] - g[1][1]) * (0.5 / RT6),
                (g[0][1] + g[1][0]) * (0.5 / RT2),
                (g[0][2] + g[2][0]) * (0.5 / RT2),
                (g[1][2] + g[2][1]) * (0.5 / RT2),
            )
        )
    stacked = [jnp.stack([p[i] for p in per], 0) for i in range(6)]
    return stacked[0], stacked[1:]


def full_tensor(mean, dev):
    side = dev[1] * (1.0 / RT6)
    return [
        mean - side + dev[0] * (1.0 / RT2),
        mean - side - dev[0] * (1.0 / RT2),
        mean + dev[1] * (2.0 / RT6),
        dev[2] * (1.0 / RT2),
        dev[3] * (1.0 / RT2),
        dev[4] * (1.0 / RT2),
    ]


SYM = ((0, 3, 4), (3, 1, 5), (4, 5, 2))


def several(step, first, number):
    def body(turn, state):
        for k in range(number):
            state = step(first + number * turn + k, state)
        return state

    return body


def material_kernel(
    count_vmem, fields, xlo, xhi, yeven, yodd, zlo, zhi, damage_ref, slip_ref, resist_ref, rows_ref, turn_ref,
    past_ref, steps_ref,
    slip_hbm, resist_hbm, tensor_out, out0, out1, out2, out3, out4, out5,
    ylo, yhi, scaled_ref, sums_ref, soft_ref, slip_out, resist_out, count_ref, sent, told,
):
    nx, ny = fields.shape[1], fields.shape[2]
    odd = parity()
    row_even, row_odd = (1 - odd) * (ny - 1), odd * (ny - 1)
    oxlo, oxhi, oyeven, oyodd, ozlo, ozhi = in_order((out0, out1, out2, out3, out4, out5), ORDER_LAST)
    tell = pltpu.make_async_copy(count_vmem, count_ref, told)
    tell.start()
    sort_halos(odd, yeven, yodd, ylo, yhi)
    halos = (xlo, xhi, ylo, yhi, zlo, zhi)
    copies = []
    for x0 in range(0, nx, WIDE):
        for h in range(ny // 8):
            spot = (pl.ds(x0, WIDE), pl.ds(8 * h, 8), slice(None))
            steps = steps_ref[spot]
            count = steps.astype(jnp.float32)
            time_step = 1.0 / count
            degrade = stiffness(damage_ref[spot])
            scale = jnp.sqrt(rate_scale * degrade * time_step)
            for k in range(len(SLOTS)):
                scaled_ref[k] = rows_ref[(k,) + spot] * scale

            def entry(a, c):
                return scaled_ref[SLOT_OF[(a, c)]]

            def turned(vector):
                return [total(turn_ref[(DEV * c + d,) + spot] * vector[d] for d in range(DEV)) for c in range(DEV)]

            def returned(vector):
                return [total(turn_ref[(DEV * c + d,) + spot] * vector[c] for c in range(DEV)) for d in range(DEV)]

            def project(vector, a):
                return total(entry(a, c) * vector[c] for c in entries(a))

            def gather(weights, c):
                return chain(entry(a, c) * weights[a] for a in range(SLIP) if c in entries(a))

            trace_u, strain = strain_parts(fields, halos, 0, x0, h)
            strain = turned(strain)
            lift = jnp.sqrt(degrade * count * (1.0 / rate_scale))
            drive = tuple(lift * (strain[c] - past_ref[(c,) + spot]) for c in range(DEV))
            grow = (rate_scale * harden_rate) * time_step
            zero = jnp.zeros_like(count)

            def rates(driving, growth):
                return [jnp.tanh(project(driving, a) / (resist_ref[(a,) + spot] + growth)) for a in range(SLIP)]

            def substep(_, state):
                driving, growth = state
                rate = rates(driving, growth)
                for a in range(SLIP):
                    sums_ref[a] = sums_ref[a] + rate[a]
                growth = growth + grow * total(jnp.abs(r) for r in rate)
                driving = tuple(driving[c] - gather(rate, c) for c in range(DEV))
                return driving, growth

            def masked(turn, state):
                driving, growth = state
                live = turn < steps
                return substep(turn, (tuple(jnp.where(live, d, 0.0) for d in driving), growth))

            for a in range(SLIP):
                sums_ref[a] = zero
            if x0 == 0 and h == 0:
                tell.wait()
            least = most = count_ref[x0, 0, 4 * h]
            for x in range(x0, x0 + WIDE):
                for j in range(4):
                    least = jnp.minimum(least, count_ref[x, 0, 4 * h + j])
                    most = jnp.maximum(most, count_ref[x, 0, 4 * h + j])
            full = lax.div(least, UNROLL)
            state = lax.fori_loop(0, full, several(substep, 0, UNROLL), (drive, zero))
            first = UNROLL * full
            rest = lax.div(most - first + (UNROLL_MASKED - 1), UNROLL_MASKED)
            _, growth = lax.fori_loop(0, rest, several(masked, first, UNROLL_MASKED), state)
            sums = [sums_ref[a] for a in range(SLIP)]
            for a in range(SLIP):
                slip_out[(a,) + spot] = slip_ref[(a,) + spot] + (rate_scale * time_step) * sums[a]
                resist_out[(a,) + spot] = resist_ref[(a,) + spot] + growth
            group = x0 // WIDE * (ny // 8) + h
            for kind, (held, away) in enumerate(((slip_out, slip_hbm), (resist_out, resist_hbm))):
                part = (slice(None),) + spot
                copy = pltpu.make_async_copy(held.at[part], away.at[part], sent.at[kind, group])
                copy.start()
                copies.append(copy)
            drive = [drive[c] - gather(sums, c) for c in range(DEV)]
            stress = returned([scale * d for d in drive])
            for a, ratio in enumerate(rates(drive, growth)):
                soft_ref[a] = (1.0 - ratio * ratio) / (resist_ref[(a,) + spot] + growth)
            bulk = degrade * (lame_first + 1.0 / 3.0)
            for k, value in enumerate(full_tensor(bulk * trace_u, stress)):
                tensor_out[(k,) + spot] = value

            def tangent(f):
                trace_v, dev = strain_parts(fields, halos, f, x0, h)
                dev = [degrade * d for d in dev]
                local = turned(dev)
                weights = [soft_ref[a] * project(local, a) for a in range(SLIP)]
                loss = returned([count * gather(weights, c) for c in range(DEV)])
                for k, value in enumerate(full_tensor(bulk * trace_v, [d - q for d, q in zip(dev, loss)])):
                    tensor_out[(6 * f + k,) + spot] = value
                return 0

            tangent(1)
            tangent(2)
    tiles = []
    for f in range(3):
        for i in range(3):
            n = 3 * f + i
            sx, sy, sz = (6 * f + SYM[i][j] for j in range(3))
            oxlo[n] = tensor_out[sx, 0]
            oxhi[n] = tensor_out[sx, nx - 1]
            for x in range(nx):
                oyeven[pl.ds(n * nx + x, 1), :] = tensor_out[sy, x, pl.ds(row_even, 1), :]
                oyodd[pl.ds(n * nx + x, 1), :] = tensor_out[sy, x, pl.ds(row_odd, 1), :]
                for h in range(ny // 8):
                    tiles.append(tensor_out[sz, x, pl.ds(8 * h, 8), :])
    ozlo[...] = pack_lane(tiles, 0)
    ozhi[...] = pack_lane(tiles, LANES - 1)
    for copy in copies:
        copy.wait()


def diverge_kernel(
    tensor_ref, xlo, xhi, yeven, yodd, zlo, zhi, force_ref, residual, tangent_a, tangent_b, ylo, yhi
):
    nx, ny = tensor_ref.shape[1], tensor_ref.shape[2]
    sort_halos(parity(), yeven, yodd, ylo, yhi)
    row_at = lax.broadcasted_iota(jnp.int32, (8, LANES), 0)
    lane_at = lax.broadcasted_iota(jnp.int32, (8, LANES), 1)
    for f, out in enumerate((residual, tangent_a, tangent_b)):
        for i in range(3):
            n = 3 * f + i
            sx, sy, sz = (6 * f + SYM[i][j] for j in range(3))
            for x in range(nx):
                for h in range(ny // 8):
                    rows = pl.ds(8 * h, 8)
                    ahead = tensor_ref[sx, x + 1, rows, :] if x + 1 < nx else xhi[n, rows, :]
                    behind = tensor_ref[sx, x - 1, rows, :] if x > 0 else xlo[n, rows, :]
                    row = n * nx + x
                    here = tensor_ref[sy, x, rows, :]
                    if 8 * h + 8 < ny:
                        over = tensor_ref[sy, x, pl.ds(8 * h + 1, 8), :]
                    else:
                        edge = jnp.broadcast_to(yhi[pl.ds(row, 1), :], (8, LANES))
                        over = jnp.where(row_at == 7, edge, pltpu.roll(here, 7, 0))
                    if h > 0:
                        under = tensor_ref[sy, x, pl.ds(8 * h - 1, 8), :]
                    else:
                        edge = jnp.broadcast_to(ylo[pl.ds(row, 1), :], (8, LANES))
                        under = jnp.where(row_at == 0, edge, pltpu.roll(here, 1, 0))
                    k = row * (ny // 8) + h
                    here = tensor_ref[sz, x, rows, :]
                    top = pltpu.roll(zhi[...], (LANES - 1 - k) % LANES, 1)
                    low = pltpu.roll(zlo[...], (LANES - k) % LANES, 1) if k else zlo[...]
                    right = jnp.where(lane_at == LANES - 1, top, pltpu.roll(here, LANES - 1, 1))
                    left = jnp.where(lane_at == 0, low, pltpu.roll(here, 1, 1))
                    value = 0.5 * ((ahead - behind) + (over - under) + (right - left))
                    if f == 0:
                        value = value + force_ref[i, x, rows, :]
                    out[i, x, rows, :] = value


def exchange(faces, order):
    def shift(value, axis, step):
        size = lax.axis_size(axis)
        return lax.ppermute(value, axis, [(i, i + step) for i in range(size) if 0 <= i + step < size])

    def swap(value, axis, first):
        size = lax.axis_size(axis)
        pairs = [(i, i + 1) for i in range(first, size - 1, 2)]
        return lax.ppermute(value, axis, pairs + [(j, i) for i, j in pairs])

    moves = {
        "xlo": lambda v: ("xhi", shift(v, "gx", -1)),
        "xhi": lambda v: ("xlo", shift(v, "gx", 1)),
        "yeven": lambda v: ("yeven", swap(v, "gy", 0)),
        "yodd": lambda v: ("yodd", swap(v, "gy", 1)),
        "zlo": lambda v: ("zhi", shift(v, "gz", -1)),
        "zhi": lambda v: ("zlo", shift(v, "gz", 1)),
    }
    got = {}
    for name, value in zip(order, faces):
        side, value = moves[name](value)
        got[side] = value
    return [got[name] for name in NAMES]


def in_hbm(value):
    return pltpu.with_memory_space_constraint(value, pltpu.HBM)


def shaped(*dims):
    return jax.ShapeDtypeStruct(dims, jnp.float32)


def on_device(displace, dir_a, dir_b, force, damage, slip, resist, grains, counts, schmid_raw):
    nx, ny, nz = damage.shape
    shape_of = {"x": shaped(9, ny, nz), "y": shaped(9 * nx, nz), "z": shaped(8, nz)}
    vmem = pl.BlockSpec(memory_space=pltpu.VMEM)
    hbm = pl.BlockSpec(memory_space=pltpu.HBM)
    params = pltpu.CompilerParams(vmem_limit_bytes=VMEM_LIMIT)
    fields, *faces = pl.pallas_call(
        faces_kernel,
        out_shape=[shaped(9, nx, ny, nz)] + [shape_of[name[0]] for name in ORDER_FIRST],
        in_specs=[hbm] * 3,
        out_specs=[vmem] * 7,
        scratch_shapes=[pltpu.SemaphoreType.DMA((3,))],
        compiler_params=params,
        name="faces",
    )(*(in_hbm(v) for v in (displace, dir_a, dir_b)))
    points = [in_hbm(v) for v in (damage, slip, resist, grains)]
    number = jnp.transpose(counts, (0, 2, 1))
    rows, turn, past, steps, *points, number = pl.pallas_call(
        table_kernel,
        out_shape=[shaped(k, nx, ny, nz) for k in (len(SLOTS), DEV * DEV, DEV)]
        + [jax.ShapeDtypeStruct((nx, ny, nz), jnp.int32)]
        + [jax.ShapeDtypeStruct(p.shape, p.dtype) for p in points]
        + [jax.ShapeDtypeStruct(number.shape, number.dtype)],
        in_specs=[hbm] * 6,
        out_specs=[vmem] * 9,
        scratch_shapes=[
            pltpu.VMEM((9, SLIP, GRAINS), jnp.float32),
            pltpu.VMEM((9, 24, LANES), jnp.float32),
            pltpu.SMEM(number.shape, jnp.int32),
            pltpu.SemaphoreType.DMA((7,)),
        ],
        compiler_params=params,
        name="table",
    )(in_hbm(jnp.transpose(schmid_raw, (2, 1, 0))), *points, in_hbm(number))
    halos = exchange(faces, ORDER_FIRST)
    groups = nx // WIDE * (ny // 8)
    outs = pl.pallas_call(
        material_kernel,
        out_shape=[shaped(SLIP, nx, ny, nz)] * 2 + [shaped(18, nx, ny, nz)]
        + [shape_of[name[0]] for name in ORDER_LAST],
        in_specs=[vmem] * 15,
        out_specs=[hbm] * 2 + [vmem] * 7,
        scratch_shapes=[
            pltpu.VMEM((9 * nx, nz), jnp.float32),
            pltpu.VMEM((9 * nx, nz), jnp.float32),
            pltpu.VMEM((len(SLOTS), WIDE, 8, LANES), jnp.float32),
            pltpu.VMEM((SLIP, WIDE, 8, LANES), jnp.float32),
            pltpu.VMEM((SLIP, WIDE, 8, LANES), jnp.float32),
            pltpu.VMEM((SLIP, nx, ny, nz), jnp.float32),
            pltpu.VMEM((SLIP, nx, ny, nz), jnp.float32),
            pltpu.SMEM(number.shape, jnp.int32),
            pltpu.SemaphoreType.DMA((2, groups)),
            pltpu.SemaphoreType.DMA,
        ],
        compiler_params=params,
        name="material",
    )(number, fields, *halos, *points[:3], rows, turn, past, steps)
    slip_new, resist_new, tensors = outs[:3]
    halos = exchange(outs[3:], ORDER_LAST)
    residual, tangent_a, tangent_b = pl.pallas_call(
        diverge_kernel,
        out_shape=[shaped(3, nx, ny, nz)] * 3,
        in_specs=[vmem] * 8,
        out_specs=[vmem] * 3,
        scratch_shapes=[pltpu.VMEM((9 * nx, nz), jnp.float32)] * 2,
        compiler_params=params,
        name="diverge",
    )(tensors, *halos, force)
    return residual, tangent_a, tangent_b, slip_new, resist_new


def solution(mesh):
    field = P(None, "gx", "gy", "gz")
    point = P("gx", "gy", "gz")
    return jax.shard_map(
        on_device,
        mesh=mesh,
        in_specs=(field, field, field, field, point, field, field, point, point, P()),
        out_specs=(field,) * 5,
        check_vma=False,
    )
```

```python
import math

import jax
import jax.numpy as jnp
from jax import lax
from jax.experimental import pallas as pl
from jax.experimental.pallas import tpu as pltpu
from jax.sharding import PartitionSpec as P

SLIP = 12
GRAINS = 64
DEV = 5
WIDE = 2
UNROLL = 4
NAMES = ("xlo", "xhi", "yeven", "yodd", "zlo", "zhi")
ORDER_FIRST = ("xlo", "xhi", "yeven", "yodd", "zlo", "zhi")
ORDER_LAST = ("yeven", "xlo", "xhi", "zlo", "zhi", "yodd")
UNROLL_MASKED = 2
LANES = 128
VMEM_LIMIT = 12 * 1024 * 1024


lame_first = 0.8
rate_scale = 1.5
harden_rate = 0.3
floor_stiff = 0.05

RT2 = math.sqrt(2.0)
RT6 = math.sqrt(6.0)


def entries(system):
    return range(min(system + 1, DEV))


SLOTS = [(a, c) for a in range(SLIP) for c in entries(a)]
SLOT_OF = {pair: k for k, pair in enumerate(SLOTS)}


def total(terms):
    terms = list(terms)
    while len(terms) > 1:
        terms = [terms[i] + terms[i + 1] if i + 1 < len(terms) else terms[i] for i in range(0, len(terms), 2)]
    return terms[0]


def chain(terms):
    terms = list(terms)
    acc = terms[0]
    for term in terms[1:]:
        acc = acc + term
    return acc


def pack_lane(tiles, lane, slots=None, packed=None):
    at = lax.broadcasted_iota(jnp.int32, (8, LANES), 1)
    packed = jnp.zeros((8, LANES), jnp.float32) if packed is None else packed
    for k, tile in zip(slots or range(len(tiles)), tiles):
        shift = (k - lane) % LANES
        moved = pltpu.roll(tile, shift, 1) if shift else tile
        packed = jnp.where(at == k, moved, packed)
    return packed


def parity():
    return lax.rem(lax.axis_index("gy"), 2)


def in_order(refs, order):
    return [refs[order.index(name)] for name in NAMES]


def faces_kernel(u_hbm, a_hbm, b_hbm, fields, *refs):
    xlo, xhi, yeven, yodd, zlo, zhi = in_order(refs[:6], ORDER_FIRST)
    sem = refs[6]
    nx, ny = fields.shape[1], fields.shape[2]
    odd = parity()
    row_even, row_odd = (1 - odd) * (ny - 1), odd * (ny - 1)
    copies = [
        pltpu.make_async_copy(ref, fields.at[pl.ds(3 * f, 3)], sem.at[f]) for f, ref in enumerate((u_hbm, a_hbm, b_hbm))
    ]
    for copy in copies:
        copy.start()
    tiles = []
    for n in range(9):
        if n % 3 == 0:
            copies[n // 3].wait()
        xlo[n] = fields[n, 0]
        xhi[n] = fields[n, nx - 1]
        for x in range(nx):
            row = n * nx + x
            yeven[pl.ds(row, 1), :] = fields[n, x, pl.ds(row_even, 1), :]
            yodd[pl.ds(row, 1), :] = fields[n, x, pl.ds(row_odd, 1), :]
            for h in range(ny // 8):
                tiles.append(fields[n, x, pl.ds(8 * h, 8), :])
    zlo[...] = pack_lane(tiles, 0)
    zhi[...] = pack_lane(tiles, LANES - 1)


def tile_counts(count_ref, x, h):
    row_at = lax.broadcasted_iota(jnp.int32, (8, LANES), 0)
    numbers = [count_ref[x, 0, 4 * h + j] for j in range(4)]
    upper = jnp.where(row_at < 2, numbers[0], numbers[1])
    lower = jnp.where(row_at < 6, numbers[2], numbers[3])
    return jnp.where(row_at < 4, upper, lower)


def stiffness(damage):
    undamaged = 1.0 - damage
    return undamaged * undamaged + floor_stiff


def table_kernel(raw_hbm, *refs):
    sources, count_hbm, (rows_ref, turn_ref, past_ref, steps_ref) = refs[:4], refs[4], refs[5:9]
    targets, count_out, raw_ref, wide_ref, count_ref, sem = refs[9:13], refs[13], refs[14], refs[15], refs[16], refs[17]
    _, slip_ref, _, grain_ref = targets
    numbers = [
        pltpu.make_async_copy(count_hbm, count_ref, sem.at[5]),
        pltpu.make_async_copy(count_hbm, count_out, sem.at[6]),
    ]
    for copy in numbers:
        copy.start()
    nx, ny = grain_ref.shape[0], grain_ref.shape[1]
    first = pltpu.make_async_copy(raw_hbm, raw_ref, sem.at[4])
    first.start()
    copies = [pltpu.make_async_copy(source, target, sem.at[k]) for k, (source, target) in enumerate(zip(sources, targets))]
    for copy in copies:
        copy.start()
    wide_ref[...] = jnp.zeros_like(wide_ref)
    first.wait()
    wide_ref[:, pl.ds(0, SLIP), pl.ds(0, GRAINS)] = raw_ref[...]
    comp = [wide_ref[i] for i in range(9)]
    base = [
        (comp[0] - comp[4]) * (1.0 / RT2),
        (2.0 * comp[8] - comp[0] - comp[4]) * (1.0 / RT6),
        (comp[1] + comp[3]) * (1.0 / RT2),
        (comp[2] + comp[6]) * (1.0 / RT2),
        (comp[5] + comp[7]) * (1.0 / RT2),
    ]
    row_at = lax.broadcasted_iota(jnp.int32, (24, LANES), 0)
    both = []
    for c in range(DEV):
        both.append(jnp.where(row_at == 16 + c, 1.0, base[c]))
    for k in range(DEV - 1):
        for j in range(k + 1, DEV):
            first, second = both[k][k : k + 1], both[j][k : k + 1]
            square = first * first + second * second
            good = square > 0.0
            scale = lax.rsqrt(jnp.where(good, square, 1.0))
            cosine = jnp.where(good, first * scale, 1.0)
            sine = jnp.where(good, second * scale, 0.0)
            both[k], both[j] = cosine * both[k] + sine * both[j], cosine * both[j] - sine * both[k]
    for copy in copies + numbers:
        copy.wait()
    for x in range(nx):
        for h in range(ny // 8):
            rows = pl.ds(8 * h, 8)
            ids = grain_ref[x, rows, :]

            def look(row):
                spread = jnp.broadcast_to(row, (8, LANES))
                return jnp.take_along_axis(spread, ids, axis=1, mode="promise_in_bounds")

            steps_ref[x, rows, :] = tile_counts(count_ref, x, h)
            past = [None] * DEV
            for k, (a, c) in enumerate(SLOTS):
                value = look(both[c][a : a + 1])
                rows_ref[k, x, rows, :] = value
                term = slip_ref[a, x, rows, :] * value
                past[c] = term if past[c] is None else past[c] + term
            for c in range(DEV):
                past_ref[c, x, rows, :] = past[c]
            for c in range(DEV):
                for d in range(DEV):
                    turn_ref[DEV * c + d, x, rows, :] = look(both[c][16 + d : 17 + d])


def sort_halos(odd, yeven, yodd, ylo, yhi):
    upper = odd == 0
    yhi[...] = jnp.where(upper, yeven[...], yodd[...])
    ylo[...] = jnp.where(upper, yodd[...], yeven[...])


def gradient_parts(field, halos, f, x, h):
    xlo, xhi, ylo, yhi, zlo, zhi = halos
    nx, ny = field.shape[1], field.shape[2]
    row_at = lax.broadcasted_iota(jnp.int32, (8, LANES), 0)
    lane_at = lax.broadcasted_iota(jnp.int32, (8, LANES), 1)
    out = []
    for c in range(3):
        n = 3 * f + c
        here = field[n, x, pl.ds(8 * h, 8), :]
        ahead = field[n, x + 1, pl.ds(8 * h, 8), :] if x + 1 < nx else xhi[n, pl.ds(8 * h, 8), :]
        behind = field[n, x - 1, pl.ds(8 * h, 8), :] if x > 0 else xlo[n, pl.ds(8 * h, 8), :]
        row = n * nx + x
        if 8 * h + 8 < ny:
            over = field[n, x, pl.ds(8 * h + 1, 8), :]
        else:
            edge = jnp.broadcast_to(yhi[pl.ds(row, 1), :], (8, LANES))
            over = jnp.where(row_at == 7, edge, pltpu.roll(here, 7, 0))
        if h > 0:
            under = field[n, x, pl.ds(8 * h - 1, 8), :]
        else:
            edge = jnp.broadcast_to(ylo[pl.ds(row, 1), :], (8, LANES))
            under = jnp.where(row_at == 0, edge, pltpu.roll(here, 1, 0))
        k = row * (ny // 8) + h
        top = pltpu.roll(zhi[...], (LANES - 1 - k) % LANES, 1)
        low = pltpu.roll(zlo[...], (LANES - k) % LANES, 1)
        right = jnp.where(lane_at == LANES - 1, top, pltpu.roll(here, LANES - 1, 1))
        left = jnp.where(lane_at == 0, low, pltpu.roll(here, 1, 1))
        out.append((ahead - behind, over - under, right - left))
    return out


def strain_parts(field, halos, f, x0, h):
    per = []
    for x in range(x0, x0 + WIDE):
        g = gradient_parts(field, halos, f, x, h)
        trace = (g[0][0] + g[1][1] + g[2][2]) * 0.5
        per.append(
            (
                trace,
                (g[0][0] - g[1][1]) * (0.5 / RT2),
                (2.0 * g[2][2] - g[0][0] - g[1][1]) * (0.5 / RT6),
                (g[0][1] + g[1][0]) * (0.5 / RT2),
                (g[0][2] + g[2][0]) * (0.5 / RT2),
                (g[1][2] + g[2][1]) * (0.5 / RT2),
            )
        )
    stacked = [jnp.stack([p[i] for p in per], 0) for i in range(6)]
    return stacked[0], stacked[1:]


def full_tensor(mean, dev):
    side = dev[1] * (1.0 / RT6)
    return [
        mean - side + dev[0] * (1.0 / RT2),
        mean - side - dev[0] * (1.0 / RT2),
        mean + dev[1] * (2.0 / RT6),
        dev[2] * (1.0 / RT2),
        dev[3] * (1.0 / RT2),
        dev[4] * (1.0 / RT2),
    ]


SYM = ((0, 3, 4), (3, 1, 5), (4, 5, 2))


def several(step, first, number):
    def body(turn, state):
        for k in range(number):
            state = step(first + number * turn + k, state)
        return state

    return body


def material_kernel(
    count_vmem, fields, xlo, xhi, yeven, yodd, zlo, zhi, damage_ref, slip_ref, resist_ref, rows_ref, turn_ref,
    past_ref, steps_ref,
    slip_hbm, resist_hbm, tensor_out, out0, out1, out2, out3, out4, out5,
    ylo, yhi, scaled_ref, sums_ref, soft_ref, slip_out, resist_out, count_ref, sent, told,
):
    nx, ny = fields.shape[1], fields.shape[2]
    odd = parity()
    row_even, row_odd = (1 - odd) * (ny - 1), odd * (ny - 1)
    oxlo, oxhi, oyeven, oyodd, ozlo, ozhi = in_order((out0, out1, out2, out3, out4, out5), ORDER_LAST)
    ozlo[...] = jnp.zeros_like(ozlo)
    ozhi[...] = jnp.zeros_like(ozhi)
    tell = pltpu.make_async_copy(count_vmem, count_ref, told)
    tell.start()
    sort_halos(odd, yeven, yodd, ylo, yhi)
    halos = (xlo, xhi, ylo, yhi, zlo, zhi)
    copies = []
    for x0 in range(0, nx, WIDE):
        for h in range(ny // 8):
            spot = (pl.ds(x0, WIDE), pl.ds(8 * h, 8), slice(None))
            steps = steps_ref[spot]
            count = steps.astype(jnp.float32)
            time_step = 1.0 / count
            degrade = stiffness(damage_ref[spot])
            scale = jnp.sqrt(rate_scale * degrade * time_step)
            for k in range(len(SLOTS)):
                scaled_ref[k] = rows_ref[(k,) + spot] * scale

            def entry(a, c):
                return scaled_ref[SLOT_OF[(a, c)]]

            def turned(vector):
                return [total(turn_ref[(DEV * c + d,) + spot] * vector[d] for d in range(DEV)) for c in range(DEV)]

            def returned(vector):
                return [total(turn_ref[(DEV * c + d,) + spot] * vector[c] for c in range(DEV)) for d in range(DEV)]

            def project(vector, a):
                return total(entry(a, c) * vector[c] for c in entries(a))

            def gather(weights, c):
                return chain(entry(a, c) * weights[a] for a in range(SLIP) if c in entries(a))

            trace_u, strain = strain_parts(fields, halos, 0, x0, h)
            strain = turned(strain)
            lift = jnp.sqrt(degrade * count * (1.0 / rate_scale))
            drive = tuple(lift * (strain[c] - past_ref[(c,) + spot]) for c in range(DEV))
            grow = (rate_scale * harden_rate) * time_step
            zero = jnp.zeros_like(count)

            def rates(driving, growth):
                return [jnp.tanh(project(driving, a) / (resist_ref[(a,) + spot] + growth)) for a in range(SLIP)]

            def substep(_, state):
                driving, growth = state
                rate = rates(driving, growth)
                for a in range(SLIP):
                    sums_ref[a] = sums_ref[a] + rate[a]
                growth = growth + grow * total(jnp.abs(r) for r in rate)
                driving = tuple(driving[c] - gather(rate, c) for c in range(DEV))
                return driving, growth

            def masked(turn, state):
                driving, growth = state
                live = turn < steps
                return substep(turn, (tuple(jnp.where(live, d, 0.0) for d in driving), growth))

            for a in range(SLIP):
                sums_ref[a] = zero
            if x0 == 0 and h == 0:
                tell.wait()
            least = most = count_ref[x0, 0, 4 * h]
            for x in range(x0, x0 + WIDE):
                for j in range(4):
                    least = jnp.minimum(least, count_ref[x, 0, 4 * h + j])
                    most = jnp.maximum(most, count_ref[x, 0, 4 * h + j])
            full = lax.div(least, UNROLL)
            state = lax.fori_loop(0, full, several(substep, 0, UNROLL), (drive, zero))
            first = UNROLL * full
            rest = lax.div(most - first + (UNROLL_MASKED - 1), UNROLL_MASKED)
            _, growth = lax.fori_loop(0, rest, several(masked, first, UNROLL_MASKED), state)
            sums = [sums_ref[a] for a in range(SLIP)]
            for a in range(SLIP):
                slip_out[(a,) + spot] = slip_ref[(a,) + spot] + (rate_scale * time_step) * sums[a]
                resist_out[(a,) + spot] = resist_ref[(a,) + spot] + growth
            group = x0 // WIDE * (ny // 8) + h
            for kind, (held, away) in enumerate(((slip_out, slip_hbm), (resist_out, resist_hbm))):
                part = (slice(None),) + spot
                copy = pltpu.make_async_copy(held.at[part], away.at[part], sent.at[kind, group])
                copy.start()
                copies.append(copy)
            drive = [drive[c] - gather(sums, c) for c in range(DEV)]
            stress = returned([scale * d for d in drive])
            for a, ratio in enumerate(rates(drive, growth)):
                soft_ref[a] = (1.0 - ratio * ratio) / (resist_ref[(a,) + spot] + growth)
            bulk = degrade * (lame_first + 1.0 / 3.0)
            for k, value in enumerate(full_tensor(bulk * trace_u, stress)):
                tensor_out[(k,) + spot] = value

            def tangent(f):
                trace_v, dev = strain_parts(fields, halos, f, x0, h)
                dev = [degrade * d for d in dev]
                local = turned(dev)
                weights = [soft_ref[a] * project(local, a) for a in range(SLIP)]
                loss = returned([count * gather(weights, c) for c in range(DEV)])
                for k, value in enumerate(full_tensor(bulk * trace_v, [d - q for d, q in zip(dev, loss)])):
                    tensor_out[(6 * f + k,) + spot] = value
                return 0

            tangent(1)
            tangent(2)
            slots, tiles = [], []
            for n in range(9):
                for x in range(x0, x0 + WIDE):
                    slots.append((n * nx + x) * (ny // 8) + h)
                    tiles.append(tensor_out[6 * (n // 3) + SYM[n % 3][2], x, pl.ds(8 * h, 8), :])
            ozlo[...] = pack_lane(tiles, 0, slots, ozlo[...])
            ozhi[...] = pack_lane(tiles, LANES - 1, slots, ozhi[...])
    for f in range(3):
        for i in range(3):
            n = 3 * f + i
            sx, sy = (6 * f + SYM[i][j] for j in range(2))
            oxlo[n] = tensor_out[sx, 0]
            oxhi[n] = tensor_out[sx, nx - 1]
            for x in range(nx):
                oyeven[pl.ds(n * nx + x, 1), :] = tensor_out[sy, x, pl.ds(row_even, 1), :]
                oyodd[pl.ds(n * nx + x, 1), :] = tensor_out[sy, x, pl.ds(row_odd, 1), :]
    for copy in copies:
        copy.wait()


def diverge_kernel(
    tensor_ref, xlo, xhi, yeven, yodd, zlo, zhi, force_ref, residual, tangent_a, tangent_b, ylo, yhi
):
    nx, ny = tensor_ref.shape[1], tensor_ref.shape[2]
    sort_halos(parity(), yeven, yodd, ylo, yhi)
    row_at = lax.broadcasted_iota(jnp.int32, (8, LANES), 0)
    lane_at = lax.broadcasted_iota(jnp.int32, (8, LANES), 1)
    for f, out in enumerate((residual, tangent_a, tangent_b)):
        for i in range(3):
            n = 3 * f + i
            sx, sy, sz = (6 * f + SYM[i][j] for j in range(3))
            for x in range(nx):
                for h in range(ny // 8):
                    rows = pl.ds(8 * h, 8)
                    ahead = tensor_ref[sx, x + 1, rows, :] if x + 1 < nx else xhi[n, rows, :]
                    behind = tensor_ref[sx, x - 1, rows, :] if x > 0 else xlo[n, rows, :]
                    row = n * nx + x
                    here = tensor_ref[sy, x, rows, :]
                    if 8 * h + 8 < ny:
                        over = tensor_ref[sy, x, pl.ds(8 * h + 1, 8), :]
                    else:
                        edge = jnp.broadcast_to(yhi[pl.ds(row, 1), :], (8, LANES))
                        over = jnp.where(row_at == 7, edge, pltpu.roll(here, 7, 0))
                    if h > 0:
                        under = tensor_ref[sy, x, pl.ds(8 * h - 1, 8), :]
                    else:
                        edge = jnp.broadcast_to(ylo[pl.ds(row, 1), :], (8, LANES))
                        under = jnp.where(row_at == 0, edge, pltpu.roll(here, 1, 0))
                    k = row * (ny // 8) + h
                    here = tensor_ref[sz, x, rows, :]
                    top = pltpu.roll(zhi[...], (LANES - 1 - k) % LANES, 1)
                    low = pltpu.roll(zlo[...], (LANES - k) % LANES, 1) if k else zlo[...]
                    right = jnp.where(lane_at == LANES - 1, top, pltpu.roll(here, LANES - 1, 1))
                    left = jnp.where(lane_at == 0, low, pltpu.roll(here, 1, 1))
                    value = 0.5 * ((ahead - behind) + (over - under) + (right - left))
                    if f == 0:
                        value = value + force_ref[i, x, rows, :]
                    out[i, x, rows, :] = value


def exchange(faces, order):
    def shift(value, axis, step):
        size = lax.axis_size(axis)
        return lax.ppermute(value, axis, [(i, i + step) for i in range(size) if 0 <= i + step < size])

    def swap(value, axis, first):
        size = lax.axis_size(axis)
        pairs = [(i, i + 1) for i in range(first, size - 1, 2)]
        return lax.ppermute(value, axis, pairs + [(j, i) for i, j in pairs])

    moves = {
        "xlo": lambda v: ("xhi", shift(v, "gx", -1)),
        "xhi": lambda v: ("xlo", shift(v, "gx", 1)),
        "yeven": lambda v: ("yeven", swap(v, "gy", 0)),
        "yodd": lambda v: ("yodd", swap(v, "gy", 1)),
        "zlo": lambda v: ("zhi", shift(v, "gz", -1)),
        "zhi": lambda v: ("zlo", shift(v, "gz", 1)),
    }
    got = {}
    for name, value in zip(order, faces):
        side, value = moves[name](value)
        got[side] = value
    return [got[name] for name in NAMES]


def in_hbm(value):
    return pltpu.with_memory_space_constraint(value, pltpu.HBM)


def shaped(*dims):
    return jax.ShapeDtypeStruct(dims, jnp.float32)


def on_device(displace, dir_a, dir_b, force, damage, slip, resist, grains, counts, schmid_raw):
    nx, ny, nz = damage.shape
    shape_of = {"x": shaped(9, ny, nz), "y": shaped(9 * nx, nz), "z": shaped(8, nz)}
    vmem = pl.BlockSpec(memory_space=pltpu.VMEM)
    hbm = pl.BlockSpec(memory_space=pltpu.HBM)
    params = pltpu.CompilerParams(vmem_limit_bytes=VMEM_LIMIT)
    fields, *faces = pl.pallas_call(
        faces_kernel,
        out_shape=[shaped(9, nx, ny, nz)] + [shape_of[name[0]] for name in ORDER_FIRST],
        in_specs=[hbm] * 3,
        out_specs=[vmem] * 7,
        scratch_shapes=[pltpu.SemaphoreType.DMA((3,))],
        compiler_params=params,
        name="faces",
    )(*(in_hbm(v) for v in (displace, dir_a, dir_b)))
    points = [in_hbm(v) for v in (damage, slip, resist, grains)]
    number = jnp.transpose(counts, (0, 2, 1))
    rows, turn, past, steps, *points, number = pl.pallas_call(
        table_kernel,
        out_shape=[shaped(k, nx, ny, nz) for k in (len(SLOTS), DEV * DEV, DEV)]
        + [jax.ShapeDtypeStruct((nx, ny, nz), jnp.int32)]
        + [jax.ShapeDtypeStruct(p.shape, p.dtype) for p in points]
        + [jax.ShapeDtypeStruct(number.shape, number.dtype)],
        in_specs=[hbm] * 6,
        out_specs=[vmem] * 9,
        scratch_shapes=[
            pltpu.VMEM((9, SLIP, GRAINS), jnp.float32),
            pltpu.VMEM((9, 24, LANES), jnp.float32),
            pltpu.SMEM(number.shape, jnp.int32),
            pltpu.SemaphoreType.DMA((7,)),
        ],
        compiler_params=params,
        name="table",
    )(in_hbm(jnp.transpose(schmid_raw, (2, 1, 0))), *points, in_hbm(number))
    halos = exchange(faces, ORDER_FIRST)
    groups = nx // WIDE * (ny // 8)
    outs = pl.pallas_call(
        material_kernel,
        out_shape=[shaped(SLIP, nx, ny, nz)] * 2 + [shaped(18, nx, ny, nz)]
        + [shape_of[name[0]] for name in ORDER_LAST],
        in_specs=[vmem] * 15,
        out_specs=[hbm] * 2 + [vmem] * 7,
        scratch_shapes=[
            pltpu.VMEM((9 * nx, nz), jnp.float32),
            pltpu.VMEM((9 * nx, nz), jnp.float32),
            pltpu.VMEM((len(SLOTS), WIDE, 8, LANES), jnp.float32),
            pltpu.VMEM((SLIP, WIDE, 8, LANES), jnp.float32),
            pltpu.VMEM((SLIP, WIDE, 8, LANES), jnp.float32),
            pltpu.VMEM((SLIP, nx, ny, nz), jnp.float32),
            pltpu.VMEM((SLIP, nx, ny, nz), jnp.float32),
            pltpu.SMEM(number.shape, jnp.int32),
            pltpu.SemaphoreType.DMA((2, groups)),
            pltpu.SemaphoreType.DMA,
        ],
        compiler_params=params,
        name="material",
    )(number, fields, *halos, *points[:3], rows, turn, past, steps)
    slip_new, resist_new, tensors = outs[:3]
    halos = exchange(outs[3:], ORDER_LAST)
    residual, tangent_a, tangent_b = pl.pallas_call(
        diverge_kernel,
        out_shape=[shaped(3, nx, ny, nz)] * 3,
        in_specs=[vmem] * 8,
        out_specs=[vmem] * 3,
        scratch_shapes=[pltpu.VMEM((9 * nx, nz), jnp.float32)] * 2,
        compiler_params=params,
        name="diverge",
    )(tensors, *halos, force)
    return residual, tangent_a, tangent_b, slip_new, resist_new


def solution(mesh):
    field = P(None, "gx", "gy", "gz")
    point = P("gx", "gy", "gz")
    return jax.shard_map(
        on_device,
        mesh=mesh,
        in_specs=(field, field, field, field, point, field, field, point, point, P()),
        out_specs=(field,) * 5,
        check_vma=False,
    )
```
